32 devices in a mesh: grp: 4 (over z), au: 4 (over x, core), vert: 2 (over y).
Axes of the slice: x: 2, y: 2, z: 4, core: 2. Of those that a mesh axis runs over, the one named last changes fastest.
Arguments:
- visibility: float32 [8192, 2], P(('grp', 'au', 'vert')), may hold values from -6 to 6
- destination: int32 [8192, 1], P(('grp', 'au', 'vert')), may hold values from 0 to 7; in each aligned block of 256 rows (0 to 255, 256 to 511, ...) at most 128 rows name the same one
- tile_slot: int32 [8192], P(('grp', 'au', 'vert')), may hold values from 0 to 63
- offsets: int32 [8192, 2], P(('grp', 'au', 'vert')), may hold values from 0 to 120
- taper: float32 [8], replicated, may hold values from 0.2 to 1
Outputs:
- dirty_facet: float32 [512, 512], P(('grp', 'au', 'vert'))
The draws below stay inside these ranges and needn't reach their ends.
Inputs may be any that keep to these rules, and one draw needn't show every extreme that they name: `destination`: among the rows of one device (aligned blocks of 256 rows) no grid block is named more than 128 times, and in some blocks one is named exactly 128 times. `tile_slot`: A tile number within the owning grid block. `offsets`: the kernel's 8 taps stay inside the tile.
All inputs are finite; a program needn't handle non-finite values.
Results may differ from the reference program's by a relative error of at most 0.0003.
Values sent between devices are 32-bit elements.
A program may use at most 64 MiB of HBM per device.

```python
import math
import jax
import jax.numpy as jnp
import numpy as np
from jax import lax

TILE = 128
SUP = 8
ROWS_DEV = 2048
COLS_DEV = 512
VIS_DEV = 256
IMG = 512
NU = 8192
NV = 1024
CAP = 128
VIS_TOTAL = 8192
TILES_DEV = 64
N_AU = 4
N_VERT = 2


def plant(result, own_key, smallest, top_value):
    extent = result.shape
    place = [jax.random.randint(jax.random.fold_in(own_key, axis), (), 0, extent[axis]) for axis in range(len(extent))]
    result = result.at[tuple(place)].set(smallest)
    longest = extent.index(max(extent))
    place[longest] = (place[longest] + 1) % extent[longest]
    return result.at[tuple(place)].set(top_value)


def block_scale(own_key, extent, cuts, low, top_value):
    loudness = 1.0
    for dim, parts in cuts:
        heights = jax.random.uniform(jax.random.fold_in(jax.random.fold_in(own_key, 6), dim), (parts,), jnp.float32, low / len(cuts), top_value / len(cuts))
        loudness = loudness * jnp.repeat(jnp.exp(heights), extent[dim] // parts).reshape((-1,) + (1,) * (len(extent) - 1 - dim))
    return loudness


def shared_out(stream_key, own, number, rows, number_of, top, bound, lean):
    order = jax.random.permutation(stream_key, number_of)
    packed, ordinary = load_shares(number_of, rows * top, bound, lean, True), load_shares(number_of, rows * top, bound, lean, False)
    places = jnp.arange(number_of)

    def named(tallies, offset_by):
        used = int((tallies > 0).sum())
        fixed = max(1, used // 4)
        shifted = fixed + (places - fixed + offset_by * (used - fixed)) % max(1, number_of - fixed)
        return jnp.zeros((number_of,), jnp.int32).at[order[jnp.where(places < fixed, places, shifted)]].set(jnp.asarray(tallies, jnp.int32))

    tallies = jnp.where(number % 4 == 0, named(packed, number // 4), named(ordinary, number - number // 4 - 1))
    mixed = jax.random.permutation(jax.random.fold_in(own, 3), number_of)
    source_of, taker = mixed[0:number_of // 2 * 2:2], mixed[1:number_of // 2 * 2:2]
    slack = jnp.minimum(tallies[source_of] - 1, bound - tallies[taker]) // 2
    slack = jnp.where((source_of == order[0]) | (taker == order[0]) | (tallies[taker] == 0), 0, jnp.maximum(slack, 0))
    shifted = jax.random.randint(jax.random.fold_in(own, 4), (number_of // 2,), 0, 1 << 20) % (slack + 1)
    tallies = tallies.at[source_of].add(-shifted).at[taker].add(shifted)
    members = jnp.searchsorted(jnp.cumsum(tallies), jnp.arange(rows * top), side="right").astype(jnp.int32)
    grid = members.reshape(top, rows).T
    grid = grid[jax.random.permutation(jax.random.fold_in(own, 1), rows)]
    offset_by = jax.random.randint(jax.random.fold_in(own, 2), (rows, 1), 0, top)
    return jnp.take_along_axis(grid, (jnp.arange(top)[None, :] + offset_by) % top, axis=1)


def load_shares(count, total, reach, slope, full):
    loads = [(1 << 20) // math.isqrt(grade ** slope) + 1 for grade in range(1, count + 1)]
    largest = reach if full else min(reach, max(-(-total // count), total * loads[0] // sum(loads)))
    least = 1 if total - largest >= count - 1 else 0
    given, rest = [largest] + [least] * (count - 1), total - largest - least * (count - 1)
    while rest > 0:
        free = [i for i in range(1, count) if given[i] < largest] or [i for i in range(1, count) if given[i] < reach]
        pool, budget = sum([loads[i] for i in free]), rest
        for i in free:
            extra = min(reach - given[i], max(1, budget * loads[i] // pool), rest)
            given[i] = given[i] + extra
            rest = rest - extra
    return np.array(given)


def normal_values(key, dims, scale, bound, pieces=(), held_as=jnp.bfloat16):
    array = jax.random.normal(key, dims, jnp.float32) * scale
    if len(pieces) > 0:
        array = block_scale(key, dims, pieces, -0.22, 0.18) * array
    return jnp.clip(array, min=-bound, max=bound).astype(held_as)


def setup_inputs(seed: int = 0) -> dict:
    streams_of = jax.random.split(jax.random.key(seed), 6)
    visibility = normal_values(streams_of[0], (VIS_TOTAL, 2), 1.0, 6.0, ((0, 32),), jnp.float32)
    destination_keys = jax.random.split(jax.random.fold_in(streams_of[1], 1), VIS_TOTAL // VIS_DEV)
    destination_turns = jax.random.permutation(jax.random.fold_in(streams_of[1], 3), VIS_TOTAL // VIS_DEV)
    destination = jax.vmap(lambda own, number: shared_out(jax.random.fold_in(streams_of[1], 2), own, number, VIS_DEV, N_AU * N_VERT, 1, CAP, 2))(destination_keys, destination_turns).reshape((VIS_TOTAL, 1))
    tile_slot = plant(jax.random.randint(streams_of[2], (VIS_TOTAL,), 0, TILES_DEV), jax.random.fold_in(streams_of[2], 1), 0, TILES_DEV - 1).astype(jnp.int32)
    offsets = plant(jax.random.randint(streams_of[3], (VIS_TOTAL, 2), 0, TILE - SUP + 1), jax.random.fold_in(streams_of[3], 1), 0, TILE - SUP).astype(jnp.int32)
    taper = jnp.clip(jax.random.uniform(streams_of[4], (SUP,), jnp.float32, 0.2, 1.0), 0.2, 1.0)
    return dict(visibility=visibility, destination=destination, tile_slot=tile_slot, offsets=offsets, taper=taper)


def matmul(factor_a, factor_b):
    return jnp.dot(factor_a, factor_b, precision=lax.Precision.HIGHEST, preferred_element_type=jnp.float32)

def phases(pixels, grid_cells, modulus):
    turn_count = pixels[:, None] * (grid_cells[None, :] - modulus // 2) % modulus
    angles = turn_count.astype(jnp.float32) * (2.0 * math.pi / modulus)
    return (jnp.cos(angles), jnp.sin(angles))

def reference(visibility, destination, tile_slot, offsets, taper):
    tiles_across = COLS_DEV // TILE
    target = destination[:, 0]
    row_anchor = target // N_VERT * ROWS_DEV + tile_slot // tiles_across * TILE + offsets[:, 0]
    col_anchor = target % N_VERT * COLS_DEV + tile_slot % tiles_across * TILE + offsets[:, 1]
    tap_range = jnp.arange(SUP, dtype=jnp.int32)
    row_index = row_anchor[:, None, None] + tap_range[None, :, None]
    col_index = col_anchor[:, None, None] + tap_range[None, None, :]
    kernel = taper[:, None] * taper[None, :]
    grid_re = jnp.zeros((NU, NV), jnp.float32).at[row_index, col_index].add(visibility[:, 0, None, None] * kernel[None])
    grid_im = jnp.zeros((NU, NV), jnp.float32).at[row_index, col_index].add(visibility[:, 1, None, None] * kernel[None])
    pixels = jnp.arange(IMG, dtype=jnp.int32) - IMG // 2
    cos_v, sin_v = phases(pixels, jnp.arange(NV, dtype=jnp.int32), NV)
    part_re = matmul(grid_re, cos_v.T) - matmul(grid_im, sin_v.T)
    part_im = matmul(grid_re, sin_v.T) + matmul(grid_im, cos_v.T)
    cos_u, sin_u = phases(pixels, jnp.arange(NU, dtype=jnp.int32), NU)
    normalise = 1.0 / (SUP * math.sqrt(VIS_TOTAL))
    return (matmul(cos_u, part_re) - matmul(sin_u, part_im)) * normalise
```

```python
import functools
import math

import jax
import jax.numpy as jnp
from jax import lax
from jax.experimental import pallas as pl
from jax.experimental.pallas import tpu as pltpu
from jax.sharding import PartitionSpec as P

TILE = 128
SUP = 8
ROWS_DEV = 2048
COLS_DEV = 512
IMG = 512
LANES = 128
AXES = ("grp", "au", "vert")
MESH = pl.DeviceIdType.MESH


def turn(angle):
    x = (angle - jnp.floor(angle + 0.5)) * (0.5 * math.pi)
    x2 = x * x
    s = x * (1.0 + x2 * (-1.0 / 6 + x2 * (1.0 / 120 + x2 * (-1.0 / 5040))))
    c = 1.0 + x2 * (-0.5 + x2 * (1.0 / 24 + x2 * (-1.0 / 720 + x2 * (1.0 / 40320))))
    s, c = 2.0 * s * c, 1.0 - 2.0 * s * s
    return 1.0 - 2.0 * s * s, 2.0 * s * c


def times(a, b):
    return a[0] * b[0] - a[1] * b[1], a[0] * b[1] + a[1] * b[0]


def halves(parts):
    high = [part.astype(jnp.bfloat16) for part in parts]
    low = [(part - h.astype(jnp.float32)).astype(jnp.bfloat16) for part, h in zip(parts, high)]
    return jnp.concatenate(high + low, axis=0)


def iota(shape, dim):
    return lax.broadcasted_iota(jnp.int32, shape, dim)


def kernel(sizes, rows, vis_ref, dest_ref, slot_ref, off_ref, taper_ref, out_ref,
           own, held, acc, send_sem, recv_sem):
    n_grp, n_au, n_vert = sizes
    count = n_grp * n_au * n_vert
    g, a, v = (lax.axis_index(name) for name in AXES)
    me = (g * n_au + a) * n_vert + v
    total_rows, total_cols = ROWS_DEV * n_au, COLS_DEV * n_vert
    vis_count = vis_ref.shape[1]

    def peer(step):
        index = lax.rem(me + step, count)
        return (
            index,
            (index // (n_au * n_vert), lax.rem(index // n_vert, n_au), lax.rem(index, n_vert)),
        )

    barrier = pltpu.get_barrier_semaphore()

    @pl.loop(1, count)
    def _(step):
        pl.semaphore_signal(barrier, inc=1, device_id=peer(step)[1], device_id_type=MESH)

    across = COLS_DEV // TILE
    dest, slot = dest_ref[...], slot_ref[...]
    row0 = dest // n_vert * ROWS_DEV + slot // across * TILE + off_ref[0:1, :]
    col0 = dest % n_vert * COLS_DEV + slot % across * TILE + off_ref[1:2, :]
    own[0:2, :] = vis_ref[...]
    own[2:3, :] = (row0 - total_rows // 2).astype(jnp.float32)
    own[3:4, :] = (col0 - total_cols // 2).astype(jnp.float32)

    pad = -(-rows // 16) * 16
    blocks = IMG // LANES
    half = LANES // 2
    pixel_row = (me * rows - IMG // 2 + iota((pad, 1), 0)).astype(jnp.float32)
    tap_u = iota((pad, LANES), 1)
    tap_v = iota((SUP, IMG), 0)
    weight_u = jnp.zeros(tap_u.shape, jnp.float32)
    weight_v = jnp.zeros(tap_v.shape, jnp.float32)
    for tap in range(SUP):
        weight_u = jnp.where(tap_u == tap, taper_ref[tap], weight_u)
        weight_v = jnp.where(tap_v == tap, taper_ref[tap], weight_v)
    scale = 1.0 / (SUP * math.sqrt(vis_count * count))
    cos_u, sin_u = turn(pixel_row * tap_u.astype(jnp.float32) * (1.0 / total_rows))
    gain_u = (
        jnp.sum(weight_u * cos_u, axis=1, keepdims=True) * scale,
        jnp.sum(weight_u * sin_u, axis=1, keepdims=True) * scale,
    )
    pixel_col = (iota((SUP, IMG), 1) - IMG // 2).astype(jnp.float32)
    cos_v, sin_v = turn(pixel_col * tap_v.astype(jnp.float32) * (1.0 / total_cols))
    gain_v = (
        jnp.sum(weight_v * cos_v, axis=0, keepdims=True),
        jnp.sum(weight_v * sin_v, axis=0, keepdims=True),
    )
    eight = iota((8, 1), 0).astype(jnp.float32)
    centre = eight * LANES + (half - 0.5 - IMG // 2)

    pl.semaphore_wait(barrier, count - 1)

    def copy(slot_index, device, step):
        return pltpu.make_async_remote_copy(
            src_ref=own,
            dst_ref=held.at[slot_index],
            send_sem=send_sem.at[step],
            recv_sem=recv_sem.at[slot_index],
            device_id=device,
            device_id_type=MESH,
        )

    @pl.loop(1, count)
    def _(step):
        copy(me, peer(step)[1], step).start()

    def product(block):
        x, y = block[2:3, :], block[3:4, :]
        wave = times(turn(pixel_row * x * (1.0 / total_rows)), gain_u)
        wave = times(wave, (block[0:1, :], block[1:2, :]))
        y = y * (1.0 / total_cols)
        coarse = turn(centre * y)
        fine = turn((eight + 0.5) * y)
        steps = turn(8.0 * eight * y)
        left = [
            times(wave, (coarse[0][j : j + 1, :], coarse[1][j : j + 1, :])) for j in range(blocks)
        ]
        right = [
            times(fine, (steps[0][m : m + 1, :], steps[1][m : m + 1, :])) for m in range(half // 8)
        ]
        left = [jnp.concatenate([part[i] for part in left], axis=0) for i in (0, 1)]
        right = [jnp.concatenate([part[i] for part in right], axis=0) for i in (0, 1)]
        return lax.dot_general(
            halves(left),
            halves(right),
            (((1,), (1,)), ((), ())),
            preferred_element_type=jnp.float32,
        )

    acc[...] = product(own[...])

    @pl.loop(1, count)
    def _(step):
        source, device = peer(count - step)
        copy(source, device, step).wait_recv()
        acc[...] += product(held[source])

    top = blocks * pad
    folded = acc[: 2 * top, :] + acc[2 * top :, :]
    folded = folded[:, :LANES] + folded[:, LANES:]
    k, c = iota((LANES, LANES), 0), iota((LANES, LANES), 1)
    kk = lax.rem(k, half)
    plus = jnp.where(c == half + kk, 1.0, 0.0)
    minus = jnp.where(c == half - 1 - kk, 1.0, 0.0)
    even = jnp.where(k < half, plus + minus, 0.0)
    odd = jnp.where(k < half, 0.0, plus - minus)

    def dot(first, second):
        return jnp.dot(
            first, second, precision=lax.Precision.HIGHEST, preferred_element_type=jnp.float32
        )

    re, im = folded[:top, :], folded[top:, :]
    z_re = dot(re, even) - dot(im, odd)
    z_im = dot(im, even) + dot(re, odd)
    for j in range(blocks):
        span = slice(j * LANES, (j + 1) * LANES)
        tile = (
            z_re[j * pad : (j + 1) * pad, :] * gain_v[0][:, span]
            - z_im[j * pad : (j + 1) * pad, :] * gain_v[1][:, span]
        )
        out_ref[:, span] = tile[:rows, :]

    @pl.loop(1, count)
    def _(step):
        copy(me, peer(step)[1], step).wait_send()


def body(sizes, visibility, destination, tile_slot, offsets, taper):
    count = math.prod(sizes)
    vis_count = visibility.shape[0]
    rows = IMG // count
    pad = -(-rows // 16) * 16
    vmem = pl.BlockSpec(memory_space=pltpu.VMEM)
    return pl.pallas_call(
        functools.partial(kernel, sizes, rows),
        out_shape=jax.ShapeDtypeStruct((rows, IMG), jnp.float32),
        in_specs=[vmem] * 4 + [pl.BlockSpec(memory_space=pltpu.SMEM)],
        out_specs=vmem,
        scratch_shapes=[
            pltpu.VMEM((4, vis_count), jnp.float32),
            pltpu.VMEM((count, 4, vis_count), jnp.float32),
            pltpu.VMEM((4 * (IMG // LANES) * pad, 2 * LANES), jnp.float32),
            pltpu.SemaphoreType.DMA((count,)),
            pltpu.SemaphoreType.DMA((count,)),
        ],
        compiler_params=pltpu.CompilerParams(collective_id=0, has_side_effects=True),
        name="direct_facet",
    )(
        visibility.T,
        destination.reshape(1, vis_count),
        tile_slot.reshape(1, vis_count),
        offsets.T,
        taper,
    )


def solution(mesh):
    return jax.shard_map(
        functools.partial(body, tuple(mesh.shape[name] for name in AXES)),
        mesh=mesh,
        in_specs=(P(AXES, None), P(AXES, None), P(AXES), P(AXES, None), P()),
        out_specs=P(AXES, None),
        check_vma=False,
    )
```

```python
import functools
import math

import jax
import jax.numpy as jnp
from jax import lax
from jax.experimental import pallas as pl
from jax.experimental.pallas import tpu as pltpu
from jax.sharding import PartitionSpec as P

TILE = 128
SUP = 8
ROWS_DEV = 2048
COLS_DEV = 512
IMG = 512
LANES = 128
AXES = ("grp", "au", "vert")
MESH = pl.DeviceIdType.MESH


def turn(angle):
    x = (angle - jnp.floor(angle + 0.5)) * (0.5 * math.pi)
    x2 = x * x
    s = x * (1.0 + x2 * (-1.0 / 6 + x2 * (1.0 / 120 + x2 * (-1.0 / 5040))))
    c = 1.0 + x2 * (-0.5 + x2 * (1.0 / 24 + x2 * (-1.0 / 720 + x2 * (1.0 / 40320))))
    s, c = 2.0 * s * c, 1.0 - 2.0 * s * s
    return 1.0 - 2.0 * s * s, 2.0 * s * c


def times(a, b):
    return a[0] * b[0] - a[1] * b[1], a[0] * b[1] + a[1] * b[0]


def halves(parts):
    high = [part.astype(jnp.bfloat16) for part in parts]
    low = [(part - h.astype(jnp.float32)).astype(jnp.bfloat16) for part, h in zip(parts, high)]
    return jnp.concatenate(high + low, axis=0)


def iota(shape, dim):
    return lax.broadcasted_iota(jnp.int32, shape, dim)


def offsets_near_first(sizes):
    n_grp, n_au, n_vert = sizes
    cores = 2 if n_au % 2 == 0 else 1
    ring = sorted(range(n_grp), key=lambda s: min(s, n_grp - s))
    return [
        (s_grp, s_chip, s_vert, s_core)
        for s_grp in ring
        for s_chip in range(n_au // cores)
        for s_vert in range(n_vert)
        for s_core in range(cores)
    ]


def arrival_groups(sizes):
    plane = sizes[1] * sizes[2]
    bounds = [1]
    while bounds[-1] * 2 < plane:
        bounds.append(bounds[-1] * 2)
    bounds += [plane * k for k in range(1, sizes[0] + 1)]
    bounds = sorted(set(bounds))
    return list(zip(bounds[:-1], bounds[1:]))


def kernel(sizes, rows, vis_hbm, dest_hbm, slot_hbm, off_hbm, taper_hbm, out_ref,
           vis_ref, dest_ref, slot_ref, off_ref, taper_ref, held, acc, load_sem, send_sem, recv_sem):
    n_grp, n_au, n_vert = sizes
    count = n_grp * n_au * n_vert
    g, a, v = (lax.axis_index(name) for name in AXES)
    me = (g * n_au + a) * n_vert + v
    total_rows, total_cols = ROWS_DEV * n_au, COLS_DEV * n_vert
    vis_count = vis_ref.shape[1]

    loads = [
        pltpu.make_async_copy(src, dst, load_sem.at[i])
        for i, (src, dst) in enumerate(
            [
                (vis_hbm, vis_ref),
                (dest_hbm, dest_ref),
                (slot_hbm, slot_ref),
                (off_hbm, off_ref),
                (taper_hbm, taper_ref),
            ]
        )
    ]
    for load in loads:
        load.start()

    cores = 2 if n_au % 2 == 0 else 1
    chips = n_au // cores
    chip, core = a // cores, lax.rem(a, cores)
    to_grp = [lax.rem(g + s, n_grp) for s in range(n_grp)]
    to_chip = [lax.rem(chip + s, chips) * cores for s in range(chips)]
    to_core = [lax.rem(core + s, cores) for s in range(cores)]
    to_vert = [lax.rem(v + s, n_vert) for s in range(n_vert)]
    peers = [
        (to_grp[s_grp], to_chip[s_chip] + to_core[s_core], to_vert[s_vert])
        for s_grp, s_chip, s_vert, s_core in offsets_near_first(sizes)
    ]

    barrier = pltpu.get_barrier_semaphore()
    for peer in peers[:0:-1]:
        pl.semaphore_signal(barrier, inc=1, device_id=peer, device_id_type=MESH)
    for load in loads:
        load.wait()

    across = COLS_DEV // TILE
    dest, slot = dest_ref[...], slot_ref[...]
    row0 = dest // n_vert * ROWS_DEV + slot // across * TILE + off_ref[0:1, :]
    col0 = dest % n_vert * COLS_DEV + slot % across * TILE + off_ref[1:2, :]
    held[0, 0:2, :] = vis_ref[...]
    held[0, 2:3, :] = (row0 - total_rows // 2).astype(jnp.float32)
    held[0, 3:4, :] = (col0 - total_cols // 2).astype(jnp.float32)

    pad = -(-rows // 16) * 16
    blocks = IMG // LANES
    half = LANES // 2
    pixel_row = (me * rows - IMG // 2 + iota((pad, 1), 0)).astype(jnp.float32)
    tap_u = iota((pad, LANES), 1)
    tap_v = iota((SUP, IMG), 0)
    weight_u = jnp.zeros(tap_u.shape, jnp.float32)
    weight_v = jnp.zeros(tap_v.shape, jnp.float32)
    for tap in range(SUP):
        weight_u = jnp.where(tap_u == tap, taper_ref[tap], weight_u)
        weight_v = jnp.where(tap_v == tap, taper_ref[tap], weight_v)
    scale = 1.0 / (SUP * math.sqrt(vis_count * count))
    cos_u, sin_u = turn(pixel_row * tap_u.astype(jnp.float32) * (1.0 / total_rows))
    gain_u = (
        jnp.sum(weight_u * cos_u, axis=1, keepdims=True) * scale,
        jnp.sum(weight_u * sin_u, axis=1, keepdims=True) * scale,
    )
    pixel_col = (iota((SUP, IMG), 1) - IMG // 2).astype(jnp.float32)
    cos_v, sin_v = turn(pixel_col * tap_v.astype(jnp.float32) * (1.0 / total_cols))
    gain_v = (
        jnp.sum(weight_v * cos_v, axis=0, keepdims=True),
        jnp.sum(weight_v * sin_v, axis=0, keepdims=True),
    )
    eight = iota((8, 1), 0)
    fine_row = eight.astype(jnp.float32) + 0.5
    centre = (eight * LANES).astype(jnp.float32) + (half - 0.5 - IMG // 2)
    stride = 8.0 * (eight - (blocks - 1)).astype(jnp.float32)
    mixed_row = jnp.where(eight < blocks, centre, stride)

    pl.semaphore_wait(barrier, count - 1)

    groups = arrival_groups(sizes)
    for number, (first, last) in reversed(list(enumerate(groups))):
        for index in range(first, last):
            pltpu.make_async_remote_copy(
                src_ref=held.at[0],
                dst_ref=held.at[index],
                send_sem=send_sem,
                recv_sem=recv_sem.at[number],
                device_id=peers[index],
                device_id_type=MESH,
            ).start()

    def landed(first, last, sem):
        span = held.at[pl.ds(first, last - first)]
        return pltpu.make_async_copy(span, span, sem)

    def product(block):
        x, y = block[2:3, :], block[3:4, :]
        wave = times(turn(pixel_row * x * (1.0 / total_rows)), gain_u)
        wave = times(wave, (block[0:1, :], block[1:2, :]))
        y = y * (1.0 / total_cols)
        mixed = turn(mixed_row * y)

        def row(j):
            return mixed[0][j : j + 1, :], mixed[1][j : j + 1, :]

        left = [times(wave, row(j)) for j in range(blocks)]
        right = [turn(fine_row * y)]
        right += [times(right[0], row(j)) for j in range(blocks, 7)]
        right += [times(part, row(7)) for part in right]
        left = [jnp.concatenate([part[i] for part in left], axis=0) for i in (0, 1)]
        right = [jnp.concatenate([part[i] for part in right], axis=0) for i in (0, 1)]
        return lax.dot_general(
            halves(left),
            halves(right),
            (((1,), (1,)), ((), ())),
            preferred_element_type=jnp.float32,
        )

    acc[...] = jnp.zeros_like(acc)

    @pl.loop(0, count // 2)
    def _(pair):
        for number, (first, last) in enumerate(groups):

            @pl.when(pair == first // 2)
            def _():
                landed(first, last, recv_sem.at[number]).wait()

        acc[...] += product(jnp.concatenate([held[2 * pair], held[2 * pair + 1]], axis=1))

    top = blocks * pad
    folded = acc[: 2 * top, :] + acc[2 * top :, :]
    folded = folded[:, :LANES] + folded[:, LANES:]
    k, c = iota((LANES, LANES), 0), iota((LANES, LANES), 1)
    kk = lax.rem(k, half)
    plus = jnp.where(c == half + kk, 1.0, 0.0)
    minus = jnp.where(c == half - 1 - kk, 1.0, 0.0)
    even = jnp.where(k < half, plus + minus, 0.0)
    odd = jnp.where(k < half, 0.0, plus - minus)

    def dot(first, second):
        return jnp.dot(
            first, second, precision=lax.Precision.HIGHEST, preferred_element_type=jnp.float32
        )

    re, im = folded[:top, :], folded[top:, :]
    z_re = dot(re, even) - dot(im, odd)
    z_im = dot(im, even) + dot(re, odd)
    for j in range(blocks):
        span = slice(j * LANES, (j + 1) * LANES)
        tile = (
            z_re[j * pad : (j + 1) * pad, :] * gain_v[0][:, span]
            - z_im[j * pad : (j + 1) * pad, :] * gain_v[1][:, span]
        )
        out_ref[:, span] = tile[:rows, :]

    landed(1, count, send_sem).wait()


def body(sizes, visibility, destination, tile_slot, offsets, taper):
    count = math.prod(sizes)
    vis_count = visibility.shape[0]
    rows = IMG // count
    pad = -(-rows // 16) * 16
    vmem = pl.BlockSpec(memory_space=pltpu.VMEM)
    return pl.pallas_call(
        functools.partial(kernel, sizes, rows),
        out_shape=jax.ShapeDtypeStruct((rows, IMG), jnp.float32),
        in_specs=[pl.BlockSpec(memory_space=pl.ANY)] * 5,
        out_specs=vmem,
        scratch_shapes=[
            pltpu.VMEM((2, vis_count), jnp.float32),
            pltpu.VMEM((1, vis_count), jnp.int32),
            pltpu.VMEM((1, vis_count), jnp.int32),
            pltpu.VMEM((2, vis_count), jnp.int32),
            pltpu.SMEM((SUP,), jnp.float32),
            pltpu.VMEM((count, 4, vis_count), jnp.float32),
            pltpu.VMEM((4 * (IMG // LANES) * pad, 2 * LANES), jnp.float32),
            pltpu.SemaphoreType.DMA((5,)),
            pltpu.SemaphoreType.DMA,
            pltpu.SemaphoreType.DMA((len(arrival_groups(sizes)),)),
        ],
        compiler_params=pltpu.CompilerParams(collective_id=0, has_side_effects=True),
        name="direct_facet",
    )(
        visibility.T,
        destination.reshape(1, vis_count),
        tile_slot.reshape(1, vis_count),
        offsets.T,
        taper,
    )


def solution(mesh):
    return jax.shard_map(
        functools.partial(body, tuple(mesh.shape[name] for name in AXES)),
        mesh=mesh,
        in_specs=(P(AXES, None), P(AXES, None), P(AXES), P(AXES, None), P()),
        out_specs=P(AXES, None),
        check_vma=False,
    )
```

```python
import functools
import math

import jax
import jax.numpy as jnp
from jax import lax
from jax.experimental import pallas as pl
from jax.experimental.pallas import tpu as pltpu
from jax.sharding import PartitionSpec as P

TILE = 128
SUP = 8
ROWS_DEV = 2048
COLS_DEV = 512
IMG = 512
LANES = 128
AXES = ("grp", "au", "vert")
MESH = pl.DeviceIdType.MESH


def turn(angle):
    x = (angle - jnp.floor(angle + 0.5)) * (0.5 * math.pi)
    x2 = x * x
    s = x * (0.999994998 + x2 * (-0.166601620 + x2 * 0.008121558))
    c = 0.999999972 + x2 * (-0.499998567 + x2 * (0.041655027 + x2 * (-0.001358591)))
    s, c = 2.0 * s * c, 1.0 - 2.0 * s * s
    return 1.0 - 2.0 * s * s, 2.0 * s * c


def times(a, b):
    return a[0] * b[0] - a[1] * b[1], a[0] * b[1] + a[1] * b[0]


def halves(parts):
    high = [part.astype(jnp.bfloat16) for part in parts]
    low = [(part - h.astype(jnp.float32)).astype(jnp.bfloat16) for part, h in zip(parts, high)]
    return jnp.concatenate(high + low, axis=0)


def iota(shape, dim):
    return lax.broadcasted_iota(jnp.int32, shape, dim)


def offsets_near_first(sizes):
    n_grp, n_au, n_vert = sizes
    cores = 2 if n_au % 2 == 0 else 1
    ring = sorted(range(n_grp), key=lambda s: min(s, n_grp - s))
    return [
        (s_grp, s_chip, s_vert, s_core)
        for s_grp in ring
        for s_chip in range(n_au // cores)
        for s_vert in range(n_vert)
        for s_core in range(cores)
    ]


def arrival_groups(sizes):
    plane = sizes[1] * sizes[2]
    bounds = [1]
    while bounds[-1] * 2 < plane:
        bounds.append(bounds[-1] * 2)
    bounds += [plane * k for k in range(1, sizes[0] + 1)]
    bounds = sorted(set(bounds))
    return list(zip(bounds[:-1], bounds[1:]))


def kernel(sizes, rows, vis_hbm, dest_hbm, slot_hbm, off_hbm, taper_hbm, out_ref,
           vis_ref, dest_ref, slot_ref, off_ref, taper_ref, held, lhs, rhs, acc, load_sem, send_sem, recv_sem):
    n_grp, n_au, n_vert = sizes
    count = n_grp * n_au * n_vert
    g, a, v = (lax.axis_index(name) for name in AXES)
    me = (g * n_au + a) * n_vert + v
    total_rows, total_cols = ROWS_DEV * n_au, COLS_DEV * n_vert
    vis_count = vis_ref.shape[1]

    loads = [
        pltpu.make_async_copy(src, dst, load_sem.at[i])
        for i, (src, dst) in enumerate(
            [
                (vis_hbm, vis_ref),
                (dest_hbm, dest_ref),
                (slot_hbm, slot_ref),
                (off_hbm, off_ref),
                (taper_hbm, taper_ref),
            ]
        )
    ]
    for load in loads:
        load.start()

    cores = 2 if n_au % 2 == 0 else 1
    chips = n_au // cores
    chip, core = a // cores, lax.rem(a, cores)
    to_grp = [lax.rem(g + s, n_grp) for s in range(n_grp)]
    to_chip = [lax.rem(chip + s, chips) * cores for s in range(chips)]
    to_core = [lax.rem(core + s, cores) for s in range(cores)]
    to_vert = [lax.rem(v + s, n_vert) for s in range(n_vert)]
    peers = [
        (to_grp[s_grp], to_chip[s_chip] + to_core[s_core], to_vert[s_vert])
        for s_grp, s_chip, s_vert, s_core in offsets_near_first(sizes)
    ]

    barrier = pltpu.get_barrier_semaphore()
    for peer in peers[:0:-1]:
        pl.semaphore_signal(barrier, inc=1, device_id=peer, device_id_type=MESH)
    for load in loads:
        load.wait()

    across = COLS_DEV // TILE
    dest, slot = dest_ref[...], slot_ref[...]
    row0 = dest // n_vert * ROWS_DEV + slot // across * TILE + off_ref[0:1, :]
    col0 = dest % n_vert * COLS_DEV + slot % across * TILE + off_ref[1:2, :]
    held[0, 0:2, :] = vis_ref[...]
    held[0, 2:3, :] = (row0 - total_rows // 2).astype(jnp.float32)
    held[0, 3:4, :] = (col0 - total_cols // 2).astype(jnp.float32)

    pad = -(-rows // 16) * 16
    blocks = IMG // LANES
    half = LANES // 2
    pixel_row = (me * rows - IMG // 2 + iota((pad, 1), 0)).astype(jnp.float32)
    tap_u = iota((pad, LANES), 1)
    tap_v = iota((SUP, IMG), 0)
    weight_u = jnp.zeros(tap_u.shape, jnp.float32)
    weight_v = jnp.zeros(tap_v.shape, jnp.float32)
    for tap in range(SUP):
        weight_u = jnp.where(tap_u == tap, taper_ref[tap], weight_u)
        weight_v = jnp.where(tap_v == tap, taper_ref[tap], weight_v)
    scale = 1.0 / (SUP * math.sqrt(vis_count * count))
    cos_u, sin_u = turn(pixel_row * tap_u.astype(jnp.float32) * (1.0 / total_rows))
    gain_u = (
        jnp.sum(weight_u * cos_u, axis=1, keepdims=True) * scale,
        jnp.sum(weight_u * sin_u, axis=1, keepdims=True) * scale,
    )
    pixel_col = (iota((SUP, IMG), 1) - IMG // 2).astype(jnp.float32)
    cos_v, sin_v = turn(pixel_col * tap_v.astype(jnp.float32) * (1.0 / total_cols))
    gain_v = (
        jnp.sum(weight_v * cos_v, axis=0, keepdims=True),
        jnp.sum(weight_v * sin_v, axis=0, keepdims=True),
    )
    eight = iota((8, 1), 0)
    k, c = iota((LANES, LANES), 0), iota((LANES, LANES), 1)
    kk = lax.rem(k, half)
    plus = jnp.where(c == half + kk, 1.0, 0.0)
    minus = jnp.where(c == half - 1 - kk, 1.0, 0.0)
    even = jnp.where(k < half, plus + minus, 0.0)
    odd = jnp.where(k < half, 0.0, plus - minus)
    fine_row = eight.astype(jnp.float32) + 0.5
    centre = (eight * LANES).astype(jnp.float32) + (half - 0.5 - IMG // 2)
    mixed_v = jnp.where(eight == 4, 8.0, jnp.where(eight == 5, 16.0, 32.0))
    mixed_v = jnp.where(eight < blocks, centre, jnp.where(eight == 7, 0.0, mixed_v))
    mixed_u = jnp.where(eight == 7, 8.0, 0.0)

    def fill(buffer, part, block):
        x = block[2:3, :] * (1.0 / total_rows)
        y = block[3:4, :] * (1.0 / total_cols)
        mixed = turn(mixed_v * y + mixed_u * x)
        seeded = times(mixed, (block[0:1, :], block[1:2, :]))

        def row(pair, j):
            return pair[0][j : j + 1, :], pair[1][j : j + 1, :]

        waves = [turn(pixel_row[:8] * x)]
        for _ in range(1, pad // 8):
            waves.append(times(waves[-1], row(mixed, 7)))
        left = [times(wave, row(seeded, j)) for j in range(blocks) for wave in waves]
        right = [turn(fine_row * y)]
        for j in (4, 5, 6):
            right += [times(piece, row(mixed, j)) for piece in right]
        left = [jnp.concatenate([piece[i] for piece in left], axis=0) for i in (0, 1)]
        right = [jnp.concatenate([piece[i] for piece in right], axis=0) for i in (0, 1)]
        span = slice(part * vis_count, (part + 1) * vis_count)
        lhs[buffer, :, span] = halves(left)
        rhs[buffer, :, span] = halves(right)

    def product(buffer):
        acc[...] += lax.dot_general(
            lhs[buffer],
            rhs[buffer],
            (((1,), (1,)), ((), ())),
            preferred_element_type=jnp.float32,
        )

    acc[...] = jnp.zeros_like(acc)
    fill(0, 0, held[0])

    pl.semaphore_wait(barrier, count - 1)

    groups = arrival_groups(sizes)
    for number, (first, last) in reversed(list(enumerate(groups))):
        for index in range(first, last):
            pltpu.make_async_remote_copy(
                src_ref=held.at[0],
                dst_ref=held.at[index],
                send_sem=send_sem,
                recv_sem=recv_sem.at[number],
                device_id=peers[index],
                device_id_type=MESH,
            ).start()

    def landed(first, last, sem):
        span = held.at[pl.ds(first, last - first)]
        return pltpu.make_async_copy(span, span, sem)

    def arrive(pair):
        for number, (first, last) in enumerate(groups):
            if first == 1:
                continue

            @pl.when(pair == first // 2)
            def _():
                landed(first, last, recv_sem.at[number]).wait()

    def advance(pair, buffer):
        arrive(pair)
        product(1 - buffer)
        fill(buffer, 0, held[2 * pair])
        fill(buffer, 1, held[2 * pair + 1])

    landed(1, 2, recv_sem.at[0]).wait()
    fill(0, 1, held[1])

    @pl.loop(0, count // 4 - 1)
    def _(quad):
        advance(2 * quad + 1, 1)
        advance(2 * quad + 2, 0)

    advance(count // 2 - 1, 1)
    product(1)

    top = blocks * pad
    folded = acc[: 2 * top, :] + acc[2 * top :, :]
    folded = folded[:, :LANES] + folded[:, LANES:]
    def dot(first, second):
        return jnp.dot(
            first, second, precision=lax.Precision.HIGHEST, preferred_element_type=jnp.float32
        )

    evens, odds = dot(folded, even), dot(folded, odd)
    z_re = evens[:top, :] - odds[top:, :]
    z_im = evens[top:, :] + odds[:top, :]
    for j in range(blocks):
        span = slice(j * LANES, (j + 1) * LANES)
        here = slice(j * pad, (j + 1) * pad)
        z = times((z_re[here, :], z_im[here, :]), gain_u)
        tile = z[0] * gain_v[0][:, span] - z[1] * gain_v[1][:, span]
        out_ref[:, span] = tile[:rows, :]

    landed(1, count, send_sem).wait()


def body(sizes, visibility, destination, tile_slot, offsets, taper):
    count = math.prod(sizes)
    vis_count = visibility.shape[0]
    rows = IMG // count
    pad = -(-rows // 16) * 16
    vmem = pl.BlockSpec(memory_space=pltpu.VMEM)
    return pl.pallas_call(
        functools.partial(kernel, sizes, rows),
        out_shape=jax.ShapeDtypeStruct((rows, IMG), jnp.float32),
        in_specs=[pl.BlockSpec(memory_space=pl.ANY)] * 5,
        out_specs=vmem,
        scratch_shapes=[
            pltpu.VMEM((2, vis_count), jnp.float32),
            pltpu.VMEM((1, vis_count), jnp.int32),
            pltpu.VMEM((1, vis_count), jnp.int32),
            pltpu.VMEM((2, vis_count), jnp.int32),
            pltpu.SMEM((SUP,), jnp.float32),
            pltpu.VMEM((count, 4, vis_count), jnp.float32),
            pltpu.VMEM((2, 4 * (IMG // LANES) * pad, 2 * vis_count), jnp.bfloat16),
            pltpu.VMEM((2, 2 * LANES, 2 * vis_count), jnp.bfloat16),
            pltpu.VMEM((4 * (IMG // LANES) * pad, 2 * LANES), jnp.float32),
            pltpu.SemaphoreType.DMA((5,)),
            pltpu.SemaphoreType.DMA,
            pltpu.SemaphoreType.DMA((len(arrival_groups(sizes)),)),
        ],
        compiler_params=pltpu.CompilerParams(collective_id=0, has_side_effects=True),
        name="direct_facet",
    )(
        visibility.T,
        destination.reshape(1, vis_count),
        tile_slot.reshape(1, vis_count),
        offsets.T,
        taper,
    )


def solution(mesh):
    return jax.shard_map(
        functools.partial(body, tuple(mesh.shape[name] for name in AXES)),
        mesh=mesh,
        in_specs=(P(AXES, None), P(AXES, None), P(AXES), P(AXES, None), P()),
        out_specs=P(AXES, None),
        check_vma=False,
    )
```

```python
import functools
import math

import jax
import jax.numpy as jnp
from jax import lax
from jax.experimental import pallas as pl
from jax.experimental.pallas import tpu as pltpu
from jax.sharding import PartitionSpec as P

TILE = 128
SUP = 8
ROWS_DEV = 2048
COLS_DEV = 512
IMG = 512
LANES = 128
AXES = ("grp", "au", "vert")
MESH = pl.DeviceIdType.MESH


def turn(angle):
    x = (angle - jnp.floor(angle + 0.5)) * (0.5 * math.pi)
    x2 = x * x
    s = x * (0.999994998 + x2 * (-0.166601620 + x2 * 0.008121558))
    c = 0.999999972 + x2 * (-0.499998567 + x2 * (0.041655027 + x2 * (-0.001358591)))
    s, c = 2.0 * s * c, 1.0 - 2.0 * s * s
    return 1.0 - 2.0 * s * s, 2.0 * s * c


def times(a, b):
    return a[0] * b[0] - a[1] * b[1], a[0] * b[1] + a[1] * b[0]


def halves(parts):
    high = [part.astype(jnp.bfloat16) for part in parts]
    low = [(part - h.astype(jnp.float32)).astype(jnp.bfloat16) for part, h in zip(parts, high)]
    return jnp.concatenate(high + low, axis=0)


def iota(shape, dim):
    return lax.broadcasted_iota(jnp.int32, shape, dim)


def offsets_near_first(sizes):
    n_grp, n_au, n_vert = sizes
    cores = 2 if n_au % 2 == 0 else 1
    ring = sorted(range(n_grp), key=lambda s: min(s, n_grp - s))
    return [
        (s_grp, s_chip, s_vert, s_core)
        for s_grp in ring
        for s_chip in range(n_au // cores)
        for s_vert in range(n_vert)
        for s_core in range(cores)
    ]


def arrival_groups(sizes):
    plane = sizes[1] * sizes[2]
    bounds = [1]
    while bounds[-1] * 2 < plane:
        bounds.append(bounds[-1] * 2)
    bounds.append(plane)
    groups = list(zip(bounds[:-1], bounds[1:]))
    return groups + [(k * plane + 1, (k + 1) * plane) for k in range(1, sizes[0])]


def kernel(sizes, rows, vis_hbm, dest_hbm, slot_hbm, off_hbm, taper_hbm, out_ref,
           vis_ref, dest_ref, slot_ref, off_ref, taper_ref, held, lhs, rhs, acc, load_sem, send_sem, recv_sem, relay_sem):
    n_grp, n_au, n_vert = sizes
    count = n_grp * n_au * n_vert
    g, a, v = (lax.axis_index(name) for name in AXES)
    me = (g * n_au + a) * n_vert + v
    total_rows, total_cols = ROWS_DEV * n_au, COLS_DEV * n_vert
    vis_count = vis_ref.shape[1]

    loads = [
        pltpu.make_async_copy(src, dst, load_sem.at[i])
        for i, (src, dst) in enumerate(
            [
                (vis_hbm, vis_ref),
                (dest_hbm, dest_ref),
                (slot_hbm, slot_ref),
                (off_hbm, off_ref),
                (taper_hbm, taper_ref),
            ]
        )
    ]
    for load in loads:
        load.start()

    cores = 2 if n_au % 2 == 0 else 1
    chips = n_au // cores
    chip, core = a // cores, lax.rem(a, cores)
    to_grp = [lax.rem(g + s, n_grp) for s in range(n_grp)]
    to_chip = [lax.rem(chip + s, chips) * cores for s in range(chips)]
    to_core = [lax.rem(core + s, cores) for s in range(cores)]
    to_vert = [lax.rem(v + s, n_vert) for s in range(n_vert)]
    peers = [
        (to_grp[s_grp], to_chip[s_chip] + to_core[s_core], to_vert[s_vert])
        for s_grp, s_chip, s_vert, s_core in offsets_near_first(sizes)
    ]

    barrier = pltpu.get_barrier_semaphore()
    plane = n_au * n_vert
    along = range(plane, count, plane)
    for peer in peers[1:plane] + [peers[index] for index in along]:
        pl.semaphore_signal(barrier, inc=1, device_id=peer, device_id_type=MESH)
    for load in loads:
        load.wait()

    across = COLS_DEV // TILE
    dest, slot = dest_ref[...], slot_ref[...]
    row0 = dest // n_vert * ROWS_DEV + slot // across * TILE + off_ref[0:1, :]
    col0 = dest % n_vert * COLS_DEV + slot % across * TILE + off_ref[1:2, :]
    held[0, 0:2, :] = vis_ref[...]
    held[0, 2:3, :] = (row0 - total_rows // 2).astype(jnp.float32)
    held[0, 3:4, :] = (col0 - total_cols // 2).astype(jnp.float32)

    pad = -(-rows // 16) * 16
    blocks = IMG // LANES
    half = LANES // 2
    pixel_row = (me * rows - IMG // 2 + iota((pad, 1), 0)).astype(jnp.float32)
    tap_u = iota((pad, LANES), 1)
    tap_v = iota((SUP, IMG), 0)
    weight_u = jnp.zeros(tap_u.shape, jnp.float32)
    weight_v = jnp.zeros(tap_v.shape, jnp.float32)
    for tap in range(SUP):
        weight_u = jnp.where(tap_u == tap, taper_ref[tap], weight_u)
        weight_v = jnp.where(tap_v == tap, taper_ref[tap], weight_v)
    scale = 1.0 / (SUP * math.sqrt(vis_count * count))
    cos_u, sin_u = turn(pixel_row * tap_u.astype(jnp.float32) * (1.0 / total_rows))
    gain_u = (
        jnp.sum(weight_u * cos_u, axis=1, keepdims=True) * scale,
        jnp.sum(weight_u * sin_u, axis=1, keepdims=True) * scale,
    )
    pixel_col = (iota((SUP, IMG), 1) - IMG // 2).astype(jnp.float32)
    cos_v, sin_v = turn(pixel_col * tap_v.astype(jnp.float32) * (1.0 / total_cols))
    gain_v = (
        jnp.sum(weight_v * cos_v, axis=0, keepdims=True),
        jnp.sum(weight_v * sin_v, axis=0, keepdims=True),
    )
    eight = iota((8, 1), 0)
    k, c = iota((LANES, LANES), 0), iota((LANES, LANES), 1)
    kk = lax.rem(k, half)
    plus = jnp.where(c == half + kk, 1.0, 0.0)
    minus = jnp.where(c == half - 1 - kk, 1.0, 0.0)
    even = jnp.where(k < half, plus + minus, 0.0)
    odd = jnp.where(k < half, 0.0, plus - minus)
    fine_row = eight.astype(jnp.float32) + 0.5
    centre = (eight * LANES).astype(jnp.float32) + (half - 0.5 - IMG // 2)
    mixed_v = jnp.where(eight == 4, 8.0, jnp.where(eight == 5, 16.0, 32.0))
    mixed_v = jnp.where(eight < blocks, centre, jnp.where(eight == 7, 0.0, mixed_v))
    mixed_u = jnp.where(eight == 7, 8.0, 0.0)

    def fill(buffer, part, block):
        x = block[2:3, :] * (1.0 / total_rows)
        y = block[3:4, :] * (1.0 / total_cols)
        mixed = turn(mixed_v * y + mixed_u * x)
        seeded = times(mixed, (block[0:1, :], block[1:2, :]))

        def row(pair, j):
            return pair[0][j : j + 1, :], pair[1][j : j + 1, :]

        waves = [turn(pixel_row[:8] * x)]
        for _ in range(1, pad // 8):
            waves.append(times(waves[-1], row(mixed, 7)))
        left = [times(wave, row(seeded, j)) for j in range(blocks) for wave in waves]
        right = [turn(fine_row * y)]
        for j in (4, 5, 6):
            right += [times(piece, row(mixed, j)) for piece in right]
        left = [jnp.concatenate([piece[i] for piece in left], axis=0) for i in (0, 1)]
        right = [jnp.concatenate([piece[i] for piece in right], axis=0) for i in (0, 1)]
        span = slice(part * vis_count, (part + 1) * vis_count)
        lhs[buffer, :, span] = halves(left)
        rhs[buffer, :, span] = halves(right)

    def product(buffer):
        acc[...] += lax.dot_general(
            lhs[buffer],
            rhs[buffer],
            (((1,), (1,)), ((), ())),
            preferred_element_type=jnp.float32,
        )

    acc[...] = jnp.zeros_like(acc)
    fill(0, 0, held[0])

    pl.semaphore_wait(barrier, plane - 1 + len(along))

    groups = arrival_groups(sizes)

    def send(source, index, peer, sem):
        pltpu.make_async_remote_copy(
            src_ref=held.at[source],
            dst_ref=held.at[index],
            send_sem=send_sem,
            recv_sem=sem,
            device_id=peer,
            device_id_type=MESH,
        ).start()

    def spread_plane(base):
        for number, (first, last) in enumerate(groups):
            for index in range(first, last):
                if base <= index < base + plane:
                    send(base, index, peers[index - base], recv_sem.at[number])

    for base in along:
        send(0, base, peers[base], relay_sem.at[base // plane - 1])
    spread_plane(0)

    def landed(first, last, sem):
        span = held.at[pl.ds(first, last - first)]
        return pltpu.make_async_copy(span, span, sem)

    def arrive(pair):
        for number, (first, last) in enumerate(groups):
            if first == 1:
                continue

            if isinstance(pair, int):
                if pair == first // 2:
                    landed(first, last, recv_sem.at[number]).wait()
                continue

            @pl.when(pair == first // 2)
            def _():
                landed(first, last, recv_sem.at[number]).wait()

    def advance(pair, buffer):
        arrive(pair)
        product(1 - buffer)
        fill(buffer, 0, held[2 * pair])
        fill(buffer, 1, held[2 * pair + 1])

    landed(1, 2, recv_sem.at[0]).wait()
    fill(0, 1, held[1])

    def relay(base):
        landed(base, base + 1, relay_sem.at[base // plane - 1]).wait()
        spread_plane(base)

    for base in along[:2]:
        relay(base)
    advance(1, 1)
    for base in along[2:]:
        relay(base)
    advance(2, 0)

    @pl.loop(1, count // 4 - 1)
    def _(quad):
        advance(2 * quad + 1, 1)
        advance(2 * quad + 2, 0)

    advance(count // 2 - 1, 1)
    product(1)

    top = blocks * pad
    folded = acc[: 2 * top, :] + acc[2 * top :, :]
    folded = folded[:, :LANES] + folded[:, LANES:]
    def dot(first, second):
        return jnp.dot(
            first, second, precision=lax.Precision.HIGHEST, preferred_element_type=jnp.float32
        )

    evens, odds = dot(folded, even), dot(folded, odd)
    z_re = evens[:top, :] - odds[top:, :]
    z_im = evens[top:, :] + odds[:top, :]
    for j in range(blocks):
        span = slice(j * LANES, (j + 1) * LANES)
        here = slice(j * pad, (j + 1) * pad)
        z = times((z_re[here, :], z_im[here, :]), gain_u)
        tile = z[0] * gain_v[0][:, span] - z[1] * gain_v[1][:, span]
        out_ref[:, span] = tile[:rows, :]

    landed(1, count, send_sem).wait()


def body(sizes, visibility, destination, tile_slot, offsets, taper):
    count = math.prod(sizes)
    vis_count = visibility.shape[0]
    rows = IMG // count
    pad = -(-rows // 16) * 16
    vmem = pl.BlockSpec(memory_space=pltpu.VMEM)
    return pl.pallas_call(
        functools.partial(kernel, sizes, rows),
        out_shape=jax.ShapeDtypeStruct((rows, IMG), jnp.float32),
        in_specs=[pl.BlockSpec(memory_space=pl.ANY)] * 5,
        out_specs=vmem,
        scratch_shapes=[
            pltpu.VMEM((2, vis_count), jnp.float32),
            pltpu.VMEM((1, vis_count), jnp.int32),
            pltpu.VMEM((1, vis_count), jnp.int32),
            pltpu.VMEM((2, vis_count), jnp.int32),
            pltpu.SMEM((SUP,), jnp.float32),
            pltpu.VMEM((count, 4, vis_count), jnp.float32),
            pltpu.VMEM((2, 4 * (IMG // LANES) * pad, 2 * vis_count), jnp.bfloat16),
            pltpu.VMEM((2, 2 * LANES, 2 * vis_count), jnp.bfloat16),
            pltpu.VMEM((4 * (IMG // LANES) * pad, 2 * LANES), jnp.float32),
            pltpu.SemaphoreType.DMA((5,)),
            pltpu.SemaphoreType.DMA,
            pltpu.SemaphoreType.DMA((len(arrival_groups(sizes)),)),
            pltpu.SemaphoreType.DMA((sizes[0],)),
        ],
        compiler_params=pltpu.CompilerParams(collective_id=0, has_side_effects=True),
        name="direct_facet",
    )(
        visibility.T,
        destination.reshape(1, vis_count),
        tile_slot.reshape(1, vis_count),
        offsets.T,
        taper,
    )


def solution(mesh):
    return jax.shard_map(
        functools.partial(body, tuple(mesh.shape[name] for name in AXES)),
        mesh=mesh,
        in_specs=(P(AXES, None), P(AXES, None), P(AXES), P(AXES, None), P()),
        out_specs=P(AXES, None),
        check_vma=False,
    )
```

```python
import functools
import math

import jax
import jax.numpy as jnp
from jax import lax
from jax.experimental import pallas as pl
from jax.experimental.pallas import tpu as pltpu
from jax.sharding import PartitionSpec as P

TILE = 128
SUP = 8
ROWS_DEV = 2048
COLS_DEV = 512
IMG = 512
LANES = 128
AXES = ("grp", "au", "vert")
MESH = pl.DeviceIdType.MESH


def turn(angle):
    x = (angle - jnp.floor(angle + 0.5)) * (0.5 * math.pi)
    x2 = x * x
    s = x * (0.999994998 + x2 * (-0.166601620 + x2 * 0.008121558))
    c = 0.999999972 + x2 * (-0.499998567 + x2 * (0.041655027 + x2 * (-0.001358591)))
    s, c = 2.0 * s * c, 1.0 - 2.0 * s * s
    return 1.0 - 2.0 * s * s, 2.0 * s * c


def times(a, b):
    return a[0] * b[0] - a[1] * b[1], a[0] * b[1] + a[1] * b[0]


def halves(parts):
    high = [part.astype(jnp.bfloat16) for part in parts]
    low = [(part - h.astype(jnp.float32)).astype(jnp.bfloat16) for part, h in zip(parts, high)]
    return jnp.concatenate(high + low, axis=0)


def iota(shape, dim):
    return lax.broadcasted_iota(jnp.int32, shape, dim)


def offsets_near_first(sizes):
    n_grp, n_au, n_vert = sizes
    cores = 2 if n_au % 2 == 0 else 1
    ring = sorted(range(n_grp), key=lambda s: min(s, n_grp - s))
    return [
        (s_grp, s_chip, s_vert, s_core)
        for s_grp in ring
        for s_chip in range(n_au // cores)
        for s_vert in range(n_vert)
        for s_core in range(cores)
    ]


def arrival_groups(sizes):
    plane = sizes[1] * sizes[2]
    bounds = [1]
    while bounds[-1] * 2 < plane:
        bounds.append(bounds[-1] * 2)
    bounds += [plane * k for k in range(1, sizes[0] + 1)]
    bounds = sorted(set(bounds))
    return list(zip(bounds[:-1], bounds[1:]))


def kernel(sizes, rows, vis_hbm, dest_hbm, slot_hbm, off_hbm, taper_hbm, out_ref,
           vis_ref, dest_ref, slot_ref, off_ref, taper_ref, held, lhs, rhs, acc, load_sem, send_sem, recv_sem):
    n_grp, n_au, n_vert = sizes
    count = n_grp * n_au * n_vert
    g, a, v = (lax.axis_index(name) for name in AXES)
    me = (g * n_au + a) * n_vert + v
    total_rows, total_cols = ROWS_DEV * n_au, COLS_DEV * n_vert
    vis_count = vis_ref.shape[1]

    loads = [
        pltpu.make_async_copy(src, dst, load_sem.at[i])
        for i, (src, dst) in enumerate(
            [
                (vis_hbm, vis_ref),
                (dest_hbm, dest_ref),
                (slot_hbm, slot_ref),
                (off_hbm, off_ref),
                (taper_hbm, taper_ref),
            ]
        )
    ]
    for load in loads:
        load.start()

    cores = 2 if n_au % 2 == 0 else 1
    chips = n_au // cores
    chip, core = a // cores, lax.rem(a, cores)
    to_grp = [lax.rem(g + s, n_grp) for s in range(n_grp)]
    to_chip = [lax.rem(chip + s, chips) * cores for s in range(chips)]
    to_core = [lax.rem(core + s, cores) for s in range(cores)]
    to_vert = [lax.rem(v + s, n_vert) for s in range(n_vert)]
    peers = [
        (to_grp[s_grp], to_chip[s_chip] + to_core[s_core], to_vert[s_vert])
        for s_grp, s_chip, s_vert, s_core in offsets_near_first(sizes)
    ]

    barrier = pltpu.get_barrier_semaphore()
    for peer in peers[:0:-1]:
        pl.semaphore_signal(barrier, inc=1, device_id=peer, device_id_type=MESH)
    for load in loads:
        load.wait()

    across = COLS_DEV // TILE
    dest, slot = dest_ref[...], slot_ref[...]
    row0 = dest // n_vert * ROWS_DEV + slot // across * TILE + off_ref[0:1, :]
    col0 = dest % n_vert * COLS_DEV + slot % across * TILE + off_ref[1:2, :]
    held[0, 0:2, :] = vis_ref[...]
    held[0, 2:3, :] = (row0 - total_rows // 2).astype(jnp.float32)
    held[0, 3:4, :] = (col0 - total_cols // 2).astype(jnp.float32)

    pad = -(-rows // 16) * 16
    blocks = IMG // LANES
    half = LANES // 2
    pixel_row = (me * rows - IMG // 2 + iota((pad, 1), 0)).astype(jnp.float32)
    tap_u = iota((pad, LANES), 1)
    tap_v = iota((SUP, IMG), 0)
    weight_u = jnp.zeros(tap_u.shape, jnp.float32)
    weight_v = jnp.zeros(tap_v.shape, jnp.float32)
    for tap in range(SUP):
        weight_u = jnp.where(tap_u == tap, taper_ref[tap], weight_u)
        weight_v = jnp.where(tap_v == tap, taper_ref[tap], weight_v)
    scale = 1.0 / (SUP * math.sqrt(vis_count * count))
    cos_u, sin_u = turn(pixel_row * tap_u.astype(jnp.float32) * (1.0 / total_rows))
    gain_u = (
        jnp.sum(weight_u * cos_u, axis=1, keepdims=True) * scale,
        jnp.sum(weight_u * sin_u, axis=1, keepdims=True) * scale,
    )
    pixel_col = (iota((SUP, IMG), 1) - IMG // 2).astype(jnp.float32)
    cos_v, sin_v = turn(pixel_col * tap_v.astype(jnp.float32) * (1.0 / total_cols))
    gain_v = (
        jnp.sum(weight_v * cos_v, axis=0, keepdims=True),
        jnp.sum(weight_v * sin_v, axis=0, keepdims=True),
    )
    eight = iota((8, 1), 0)
    k, c = iota((LANES, LANES), 0), iota((LANES, LANES), 1)
    kk = lax.rem(k, half)
    plus = jnp.where(c == half + kk, 1.0, 0.0)
    minus = jnp.where(c == half - 1 - kk, 1.0, 0.0)
    even = jnp.where(k < half, plus + minus, 0.0)
    odd = jnp.where(k < half, 0.0, plus - minus)
    fine_row = eight.astype(jnp.float32) + 0.5
    centre = (eight * LANES).astype(jnp.float32) + (half - 0.5 - IMG // 2)
    mixed_v = jnp.where(eight == 4, 8.0, jnp.where(eight == 5, 16.0, 32.0))
    mixed_v = jnp.where(eight < blocks, centre, jnp.where(eight == 7, 0.0, mixed_v))
    mixed_u = jnp.where(eight == 7, 8.0, 0.0)

    def fill(buffer, part, block):
        x = block[2:3, :] * (1.0 / total_rows)
        y = block[3:4, :] * (1.0 / total_cols)
        mixed = turn(mixed_v * y + mixed_u * x)
        seeded = times(mixed, (block[0:1, :], block[1:2, :]))

        def row(pair, j):
            return pair[0][j : j + 1, :], pair[1][j : j + 1, :]

        waves = [turn(pixel_row[:8] * x)]
        for _ in range(1, pad // 8):
            waves.append(times(waves[-1], row(mixed, 7)))
        left = [times(wave, row(seeded, j)) for j in range(blocks) for wave in waves]
        right = [turn(fine_row * y)]
        for j in (4, 5, 6):
            right += [times(piece, row(mixed, j)) for piece in right]
        left = [jnp.concatenate([piece[i] for piece in left], axis=0) for i in (0, 1)]
        right = [jnp.concatenate([piece[i] for piece in right], axis=0) for i in (0, 1)]
        span = slice(part * vis_count, (part + 1) * vis_count)
        lhs[buffer, :, span] = halves(left)
        rhs[buffer, :, span] = halves(right)

    def product(buffer):
        acc[...] += lax.dot_general(
            lhs[buffer],
            rhs[buffer],
            (((1,), (1,)), ((), ())),
            preferred_element_type=jnp.float32,
        )

    acc[...] = jnp.zeros_like(acc)
    fill(0, 0, held[0])

    pl.semaphore_wait(barrier, count - 1)

    groups = arrival_groups(sizes)
    for number, (first, last) in enumerate(groups):
        for index in range(first, last):
            pltpu.make_async_remote_copy(
                src_ref=held.at[0],
                dst_ref=held.at[index],
                send_sem=send_sem,
                recv_sem=recv_sem.at[number],
                device_id=peers[index],
                device_id_type=MESH,
            ).start()

    def landed(first, last, sem):
        span = held.at[pl.ds(first, last - first)]
        return pltpu.make_async_copy(span, span, sem)

    def landing(quad):
        for number, (first, last) in enumerate(groups):
            if first < 4:
                continue

            @pl.when(quad == first // 4)
            def _():
                landed(first, last, recv_sem.at[number]).wait()

    def advance(quad, buffer):
        landing(quad)
        product(1 - buffer)
        for part in range(4):
            fill(buffer, part, held[4 * quad + part])

    for number, (first, last) in enumerate(groups):
        if first < 4:
            landed(first, last, recv_sem.at[number]).wait()
            for index in range(first, last):
                fill(0, index, held[index])

    @pl.loop(0, count // 8 - 1)
    def _(step):
        advance(2 * step + 1, 1)
        advance(2 * step + 2, 0)

    advance(count // 4 - 1, 1)
    product(1)

    top = blocks * pad
    folded = acc[: 2 * top, :] + acc[2 * top :, :]
    folded = folded[:, :LANES] + folded[:, LANES:]
    def dot(first, second):
        return jnp.dot(
            first, second, precision=lax.Precision.HIGHEST, preferred_element_type=jnp.float32
        )

    evens, odds = dot(folded, even), dot(folded, odd)
    z_re = evens[:top, :] - odds[top:, :]
    z_im = evens[top:, :] + odds[:top, :]
    for j in range(blocks):
        span = slice(j * LANES, (j + 1) * LANES)
        here = slice(j * pad, (j + 1) * pad)
        z = times((z_re[here, :], z_im[here, :]), gain_u)
        tile = z[0] * gain_v[0][:, span] - z[1] * gain_v[1][:, span]
        out_ref[:, span] = tile[:rows, :]

    landed(1, count, send_sem).wait()


def body(sizes, visibility, destination, tile_slot, offsets, taper):
    count = math.prod(sizes)
    vis_count = visibility.shape[0]
    rows = IMG // count
    pad = -(-rows // 16) * 16
    vmem = pl.BlockSpec(memory_space=pltpu.VMEM)
    return pl.pallas_call(
        functools.partial(kernel, sizes, rows),
        out_shape=jax.ShapeDtypeStruct((rows, IMG), jnp.float32),
        in_specs=[pl.BlockSpec(memory_space=pl.ANY)] * 5,
        out_specs=vmem,
        scratch_shapes=[
            pltpu.VMEM((2, vis_count), jnp.float32),
            pltpu.VMEM((1, vis_count), jnp.int32),
            pltpu.VMEM((1, vis_count), jnp.int32),
            pltpu.VMEM((2, vis_count), jnp.int32),
            pltpu.SMEM((SUP,), jnp.float32),
            pltpu.VMEM((count, 4, vis_count), jnp.float32),
            pltpu.VMEM((2, 4 * (IMG // LANES) * pad, 4 * vis_count), jnp.bfloat16),
            pltpu.VMEM((2, 2 * LANES, 4 * vis_count), jnp.bfloat16),
            pltpu.VMEM((4 * (IMG // LANES) * pad, 2 * LANES), jnp.float32),
            pltpu.SemaphoreType.DMA((5,)),
            pltpu.SemaphoreType.DMA,
            pltpu.SemaphoreType.DMA((len(arrival_groups(sizes)),)),
        ],
        compiler_params=pltpu.CompilerParams(collective_id=0, has_side_effects=True),
        name="direct_facet",
    )(
        visibility.T,
        destination.reshape(1, vis_count),
        tile_slot.reshape(1, vis_count),
        offsets.T,
        taper,
    )


def solution(mesh):
    return jax.shard_map(
        functools.partial(body, tuple(mesh.shape[name] for name in AXES)),
        mesh=mesh,
        in_specs=(P(AXES, None), P(AXES, None), P(AXES), P(AXES, None), P()),
        out_specs=P(AXES, None),
        check_vma=False,
    )
```

```python
import functools
import math

import jax
import jax.numpy as jnp
from jax import lax
from jax.experimental import pallas as pl
from jax.experimental.pallas import tpu as pltpu
from jax.sharding import PartitionSpec as P

TILE = 128
SUP = 8
ROWS_DEV = 2048
COLS_DEV = 512
IMG = 512
LANES = 128
AXES = ("grp", "au", "vert")
MESH = pl.DeviceIdType.MESH


def turn(angle):
    x = (angle - jnp.floor(angle + 0.5)) * (0.5 * math.pi)
    x2 = x * x
    s = x * (0.999994998 + x2 * (-0.166601620 + x2 * 0.008121558))
    c = 0.999999972 + x2 * (-0.499998567 + x2 * (0.041655027 + x2 * (-0.001358591)))
    s, c = 2.0 * s * c, 1.0 - 2.0 * s * s
    return 1.0 - 2.0 * s * s, 2.0 * s * c


def times(a, b):
    return a[0] * b[0] - a[1] * b[1], a[0] * b[1] + a[1] * b[0]


def halves(parts):
    high = [part.astype(jnp.bfloat16) for part in parts]
    low = [(part - h.astype(jnp.float32)).astype(jnp.bfloat16) for part, h in zip(parts, high)]
    return jnp.concatenate(high + low, axis=0)


def iota(shape, dim):
    return lax.broadcasted_iota(jnp.int32, shape, dim)


def offsets_near_first(sizes):
    n_grp, n_au, n_vert = sizes
    cores = 2 if n_au % 2 == 0 else 1
    ring = sorted(range(n_grp), key=lambda s: min(s, n_grp - s))
    return [
        (s_grp, s_chip, s_vert, s_core)
        for s_grp in ring
        for s_chip in range(n_au // cores)
        for s_vert in range(n_vert)
        for s_core in range(cores)
    ]


def arrival_groups(sizes):
    plane = sizes[1] * sizes[2]
    bounds = [1]
    while bounds[-1] * 2 < plane:
        bounds.append(bounds[-1] * 2)
    bounds += [plane * k for k in range(1, sizes[0] + 1)]
    bounds = sorted(set(bounds))
    return list(zip(bounds[:-1], bounds[1:]))


def kernel(sizes, rows, vis_hbm, dest_hbm, slot_hbm, off_hbm, taper_hbm, out_ref,
           vis_ref, dest_ref, slot_ref, off_ref, taper_ref, held, lhs, rhs, acc, load_sem, send_sem, recv_sem):
    n_grp, n_au, n_vert = sizes
    count = n_grp * n_au * n_vert
    g, a, v = (lax.axis_index(name) for name in AXES)
    me = (g * n_au + a) * n_vert + v
    total_rows, total_cols = ROWS_DEV * n_au, COLS_DEV * n_vert
    vis_count = vis_ref.shape[1]

    loads = [
        pltpu.make_async_copy(src, dst, load_sem.at[i])
        for i, (src, dst) in enumerate(
            [
                (vis_hbm, vis_ref),
                (dest_hbm, dest_ref),
                (slot_hbm, slot_ref),
                (off_hbm, off_ref),
                (taper_hbm, taper_ref),
            ]
        )
    ]
    for load in loads:
        load.start()

    cores = 2 if n_au % 2 == 0 else 1
    chips = n_au // cores
    chip, core = a // cores, lax.rem(a, cores)
    to_grp = [lax.rem(g + s, n_grp) for s in range(n_grp)]
    to_chip = [lax.rem(chip + s, chips) * cores for s in range(chips)]
    to_core = [lax.rem(core + s, cores) for s in range(cores)]
    to_vert = [lax.rem(v + s, n_vert) for s in range(n_vert)]
    peers = [
        (to_grp[s_grp], to_chip[s_chip] + to_core[s_core], to_vert[s_vert])
        for s_grp, s_chip, s_vert, s_core in offsets_near_first(sizes)
    ]

    barrier = pltpu.get_barrier_semaphore()
    for peer in peers[:0:-1]:
        pl.semaphore_signal(barrier, inc=1, device_id=peer, device_id_type=MESH)
    for load in loads:
        load.wait()

    across = COLS_DEV // TILE
    dest, slot = dest_ref[...], slot_ref[...]
    row0 = dest // n_vert * ROWS_DEV + slot // across * TILE + off_ref[0:1, :]
    col0 = dest % n_vert * COLS_DEV + slot % across * TILE + off_ref[1:2, :]
    held[0, 0:2, :] = vis_ref[...]
    held[0, 2:3, :] = (row0 - total_rows // 2).astype(jnp.float32)
    held[0, 3:4, :] = (col0 - total_cols // 2).astype(jnp.float32)

    pad = -(-rows // 16) * 16
    blocks = IMG // LANES
    half = LANES // 2
    pixel_row = (me * rows - IMG // 2 + iota((pad, 1), 0)).astype(jnp.float32)
    tap_u = iota((pad, LANES), 1)
    tap_v = iota((SUP, IMG), 0)
    weight_u = jnp.zeros(tap_u.shape, jnp.float32)
    weight_v = jnp.zeros(tap_v.shape, jnp.float32)
    for tap in range(SUP):
        weight_u = jnp.where(tap_u == tap, taper_ref[tap], weight_u)
        weight_v = jnp.where(tap_v == tap, taper_ref[tap], weight_v)
    scale = 1.0 / (SUP * math.sqrt(vis_count * count))
    cos_u, sin_u = turn(pixel_row * tap_u.astype(jnp.float32) * (1.0 / total_rows))
    gain_u = (
        jnp.sum(weight_u * cos_u, axis=1, keepdims=True) * scale,
        jnp.sum(weight_u * sin_u, axis=1, keepdims=True) * scale,
    )
    pixel_col = (iota((SUP, IMG), 1) - IMG // 2).astype(jnp.float32)
    cos_v, sin_v = turn(pixel_col * tap_v.astype(jnp.float32) * (1.0 / total_cols))
    gain_v = (
        jnp.sum(weight_v * cos_v, axis=0, keepdims=True),
        jnp.sum(weight_v * sin_v, axis=0, keepdims=True),
    )
    eight = iota((8, 1), 0)
    k, c = iota((LANES, LANES), 0), iota((LANES, LANES), 1)
    kk = lax.rem(k, half)
    plus = jnp.where(c == half + kk, 1.0, 0.0)
    minus = jnp.where(c == half - 1 - kk, 1.0, 0.0)
    even = jnp.where(k < half, plus + minus, 0.0)
    odd = jnp.where(k < half, 0.0, plus - minus)
    fine_row = eight.astype(jnp.float32) + 0.5
    centre = (eight * LANES).astype(jnp.float32) + (half - 0.5 - IMG // 2)
    mixed_v = jnp.where(eight == 4, 8.0, jnp.where(eight == 5, 16.0, 32.0))
    mixed_v = jnp.where(eight < blocks, centre, jnp.where(eight == 7, 0.0, mixed_v))
    mixed_u = jnp.where(eight == 7, 8.0, 0.0)

    def fill(buffer, part, block):
        x = block[2:3, :] * (1.0 / total_rows)
        y = block[3:4, :] * (1.0 / total_cols)
        mixed = turn(mixed_v * y + mixed_u * x)
        seeded = times(mixed, (block[0:1, :], block[1:2, :]))

        def row(pair, j):
            return pair[0][j : j + 1, :], pair[1][j : j + 1, :]

        waves = [turn(pixel_row[:8] * x)]
        for _ in range(1, pad // 8):
            waves.append(times(waves[-1], row(mixed, 7)))
        left = [times(wave, row(seeded, j)) for j in range(blocks) for wave in waves]
        right = [turn(fine_row * y)]
        for j in (4, 5, 6):
            right += [times(piece, row(mixed, j)) for piece in right]
        left = [jnp.concatenate([piece[i] for piece in left], axis=0) for i in (0, 1)]
        right = [jnp.concatenate([piece[i] for piece in right], axis=0) for i in (0, 1)]
        span = slice(part * vis_count, (part + 1) * vis_count)
        lhs[buffer, :, span] = halves(left)
        rhs[buffer, :, span] = halves(right)

    def product(buffer):
        acc[...] += lax.dot_general(
            lhs[buffer],
            rhs[buffer],
            (((1,), (1,)), ((), ())),
            preferred_element_type=jnp.float32,
        )

    acc[...] = jnp.zeros_like(acc)
    fill(0, 0, held[0])

    pl.semaphore_wait(barrier, count - 1)

    groups = arrival_groups(sizes)
    for number, (first, last) in enumerate(groups):
        for index in range(first, last):
            pltpu.make_async_remote_copy(
                src_ref=held.at[0],
                dst_ref=held.at[index],
                send_sem=send_sem,
                recv_sem=recv_sem.at[number],
                device_id=peers[index],
                device_id_type=MESH,
            ).start()

    def landed(first, last, sem):
        span = held.at[pl.ds(first, last - first)]
        return pltpu.make_async_copy(span, span, sem)

    def arrive(pair):
        for number, (first, last) in enumerate(groups):
            if first == 1:
                continue

            @pl.when(pair == first // 2)
            def _():
                landed(first, last, recv_sem.at[number]).wait()

    def advance(pair, buffer):
        arrive(pair)
        product(1 - buffer)
        fill(buffer, 0, held[2 * pair])
        fill(buffer, 1, held[2 * pair + 1])

    landed(1, 2, recv_sem.at[0]).wait()
    fill(0, 1, held[1])

    @pl.loop(0, count // 4 - 1)
    def _(quad):
        advance(2 * quad + 1, 1)
        advance(2 * quad + 2, 0)

    advance(count // 2 - 1, 1)
    product(1)

    top = blocks * pad
    folded = acc[: 2 * top, :] + acc[2 * top :, :]
    folded = folded[:, :LANES] + folded[:, LANES:]
    def dot(first, second):
        return jnp.dot(
            first, second, precision=lax.Precision.HIGHEST, preferred_element_type=jnp.float32
        )

    evens, odds = dot(folded, even), dot(folded, odd)
    z_re = evens[:top, :] - odds[top:, :]
    z_im = evens[top:, :] + odds[:top, :]
    for j in range(blocks):
        span = slice(j * LANES, (j + 1) * LANES)
        here = slice(j * pad, (j + 1) * pad)
        z = times((z_re[here, :], z_im[here, :]), gain_u)
        tile = z[0] * gain_v[0][:, span] - z[1] * gain_v[1][:, span]
        out_ref[:, span] = tile[:rows, :]

    landed(1, count, send_sem).wait()


def body(sizes, visibility, destination, tile_slot, offsets, taper):
    count = math.prod(sizes)
    vis_count = visibility.shape[0]
    rows = IMG // count
    pad = -(-rows // 16) * 16
    vmem = pl.BlockSpec(memory_space=pltpu.VMEM)
    return pl.pallas_call(
        functools.partial(kernel, sizes, rows),
        out_shape=jax.ShapeDtypeStruct((rows, IMG), jnp.float32),
        in_specs=[pl.BlockSpec(memory_space=pl.ANY)] * 5,
        out_specs=vmem,
        scratch_shapes=[
            pltpu.VMEM((2, vis_count), jnp.float32),
            pltpu.VMEM((1, vis_count), jnp.int32),
            pltpu.VMEM((1, vis_count), jnp.int32),
            pltpu.VMEM((2, vis_count), jnp.int32),
            pltpu.SMEM((SUP,), jnp.float32),
            pltpu.VMEM((count, 4, vis_count), jnp.float32),
            pltpu.VMEM((2, 4 * (IMG // LANES) * pad, 2 * vis_count), jnp.bfloat16),
            pltpu.VMEM((2, 2 * LANES, 2 * vis_count), jnp.bfloat16),
            pltpu.VMEM((4 * (IMG // LANES) * pad, 2 * LANES), jnp.float32),
            pltpu.SemaphoreType.DMA((5,)),
            pltpu.SemaphoreType.DMA,
            pltpu.SemaphoreType.DMA((len(arrival_groups(sizes)),)),
        ],
        compiler_params=pltpu.CompilerParams(collective_id=0, has_side_effects=True),
        name="direct_facet",
    )(
        visibility.T,
        destination.reshape(1, vis_count),
        tile_slot.reshape(1, vis_count),
        offsets.T,
        taper,
    )


def solution(mesh):
    return jax.shard_map(
        functools.partial(body, tuple(mesh.shape[name] for name in AXES)),
        mesh=mesh,
        in_specs=(P(AXES, None), P(AXES, None), P(AXES), P(AXES, None), P()),
        out_specs=P(AXES, None),
        check_vma=False,
    )
```

```python
import functools
import math

import jax
import jax.numpy as jnp
from jax import lax
from jax.experimental import pallas as pl
from jax.experimental.pallas import tpu as pltpu
from jax.sharding import PartitionSpec as P

TILE = 128
SUP = 8
ROWS_DEV = 2048
COLS_DEV = 512
IMG = 512
LANES = 128
AXES = ("grp", "au", "vert")
MESH = pl.DeviceIdType.MESH


def turn(angle):
    x = (angle - jnp.floor(angle + 0.5)) * (0.5 * math.pi)
    x2 = x * x
    s = x * (0.999994998 + x2 * (-0.166601620 + x2 * 0.008121558))
    c = 0.999999972 + x2 * (-0.499998567 + x2 * (0.041655027 + x2 * (-0.001358591)))
    s, c = 2.0 * s * c, 1.0 - 2.0 * s * s
    return 1.0 - 2.0 * s * s, 2.0 * s * c


def times(a, b):
    return a[0] * b[0] - a[1] * b[1], a[0] * b[1] + a[1] * b[0]


def halves(parts):
    high = [part.astype(jnp.bfloat16) for part in parts]
    low = [(part - h.astype(jnp.float32)).astype(jnp.bfloat16) for part, h in zip(parts, high)]
    return jnp.concatenate(high + low, axis=0)


def iota(shape, dim):
    return lax.broadcasted_iota(jnp.int32, shape, dim)


def offsets_near_first(sizes):
    n_grp, n_au, n_vert = sizes
    cores = 2 if n_au % 2 == 0 else 1
    ring = sorted(range(n_grp), key=lambda s: min(s, n_grp - s))
    return [
        (s_grp, s_chip, s_vert, s_core)
        for s_grp in ring
        for s_chip in range(n_au // cores)
        for s_vert in range(n_vert)
        for s_core in range(cores)
    ]


def arrival_groups(sizes):
    plane = sizes[1] * sizes[2]
    bounds = [1]
    while bounds[-1] * 2 < plane:
        bounds.append(bounds[-1] * 2)
    bounds += [plane * k for k in range(1, sizes[0] + 1)]
    bounds = sorted(set(bounds))
    return list(zip(bounds[:-1], bounds[1:]))


def kernel(sizes, rows, vis_hbm, dest_hbm, slot_hbm, off_hbm, taper_hbm, out_ref,
           vis_ref, dest_ref, slot_ref, off_ref, taper_ref, held, lhs, rhs, acc, load_sem, send_sem, recv_sem):
    n_grp, n_au, n_vert = sizes
    count = n_grp * n_au * n_vert
    g, a, v = (lax.axis_index(name) for name in AXES)
    me = (g * n_au + a) * n_vert + v
    total_rows, total_cols = ROWS_DEV * n_au, COLS_DEV * n_vert
    vis_count = vis_ref.shape[1]

    loads = [
        pltpu.make_async_copy(src, dst, load_sem.at[i])
        for i, (src, dst) in enumerate(
            [
                (vis_hbm, vis_ref),
                (dest_hbm, dest_ref),
                (slot_hbm, slot_ref),
                (off_hbm, off_ref),
                (taper_hbm, taper_ref),
            ]
        )
    ]
    for load in loads:
        load.start()

    cores = 2 if n_au % 2 == 0 else 1
    chips = n_au // cores
    chip, core = a // cores, lax.rem(a, cores)
    to_grp = [lax.rem(g + s, n_grp) for s in range(n_grp)]
    to_chip = [lax.rem(chip + s, chips) * cores for s in range(chips)]
    to_core = [lax.rem(core + s, cores) for s in range(cores)]
    to_vert = [lax.rem(v + s, n_vert) for s in range(n_vert)]
    peers = [
        (to_grp[s_grp], to_chip[s_chip] + to_core[s_core], to_vert[s_vert])
        for s_grp, s_chip, s_vert, s_core in offsets_near_first(sizes)
    ]

    barrier = pltpu.get_barrier_semaphore()
    for peer in peers[:0:-1]:
        pl.semaphore_signal(barrier, inc=1, device_id=peer, device_id_type=MESH)
    for load in loads:
        load.wait()

    across = COLS_DEV // TILE
    dest, slot = dest_ref[...], slot_ref[...]
    row0 = dest // n_vert * ROWS_DEV + slot // across * TILE + off_ref[0:1, :]
    col0 = dest % n_vert * COLS_DEV + slot % across * TILE + off_ref[1:2, :]
    held[0, 0:2, :] = vis_ref[...]
    held[0, 2:3, :] = (row0 - total_rows // 2).astype(jnp.float32)
    held[0, 3:4, :] = (col0 - total_cols // 2).astype(jnp.float32)

    pad = -(-rows // 16) * 16
    blocks = IMG // LANES
    half = LANES // 2
    pixel_row = (me * rows - IMG // 2 + iota((pad, 1), 0)).astype(jnp.float32)
    tap_u = iota((pad, LANES), 1)
    tap_v = iota((SUP, IMG), 0)
    weight_u = jnp.zeros(tap_u.shape, jnp.float32)
    weight_v = jnp.zeros(tap_v.shape, jnp.float32)
    for tap in range(SUP):
        weight_u = jnp.where(tap_u == tap, taper_ref[tap], weight_u)
        weight_v = jnp.where(tap_v == tap, taper_ref[tap], weight_v)
    scale = 1.0 / (SUP * math.sqrt(vis_count * count))
    cos_u, sin_u = turn(pixel_row * tap_u.astype(jnp.float32) * (1.0 / total_rows))
    gain_u = (
        jnp.sum(weight_u * cos_u, axis=1, keepdims=True) * scale,
        jnp.sum(weight_u * sin_u, axis=1, keepdims=True) * scale,
    )
    pixel_col = (iota((SUP, IMG), 1) - IMG // 2).astype(jnp.float32)
    cos_v, sin_v = turn(pixel_col * tap_v.astype(jnp.float32) * (1.0 / total_cols))
    gain_v = (
        jnp.sum(weight_v * cos_v, axis=0, keepdims=True),
        jnp.sum(weight_v * sin_v, axis=0, keepdims=True),
    )
    eight = iota((8, 1), 0)
    k, c = iota((LANES, LANES), 0), iota((LANES, LANES), 1)
    kk = lax.rem(k, half)
    plus = jnp.where(c == half + kk, 1.0, 0.0)
    minus = jnp.where(c == half - 1 - kk, 1.0, 0.0)
    even = jnp.where(k < half, plus + minus, 0.0)
    odd = jnp.where(k < half, 0.0, plus - minus)
    fine_row = eight.astype(jnp.float32) + 0.5
    centre = (eight * LANES).astype(jnp.float32) + (half - 0.5 - IMG // 2)
    mixed_v = jnp.where(eight == 4, 8.0, jnp.where(eight == 5, 16.0, 32.0))
    mixed_v = jnp.where(eight < blocks, centre, jnp.where(eight == 7, 0.0, mixed_v))
    mixed_u = jnp.where(eight == 7, 8.0, 0.0)

    def fill(buffer, part, block):
        x = block[2:3, :] * (1.0 / total_rows)
        y = block[3:4, :] * (1.0 / total_cols)
        mixed = turn(mixed_v * y + mixed_u * x)
        seeded = times(mixed, (block[0:1, :], block[1:2, :]))

        def row(pair, j):
            return pair[0][j : j + 1, :], pair[1][j : j + 1, :]

        waves = [turn(pixel_row[:8] * x)]
        for _ in range(1, pad // 8):
            waves.append(times(waves[-1], row(mixed, 7)))
        left = [times(wave, row(seeded, j)) for j in range(blocks) for wave in waves]
        right = [turn(fine_row * y)]
        for j in (4, 5, 6):
            right += [times(piece, row(mixed, j)) for piece in right]
        left = [jnp.concatenate([piece[i] for piece in left], axis=0) for i in (0, 1)]
        right = [jnp.concatenate([piece[i] for piece in right], axis=0) for i in (0, 1)]
        span = slice(part * vis_count, (part + 1) * vis_count)
        lhs[buffer, :, span] = halves(left)
        rhs[buffer, :, span] = halves(right)

    def product(buffer):
        acc[...] += lax.dot_general(
            lhs[buffer],
            rhs[buffer],
            (((1,), (1,)), ((), ())),
            preferred_element_type=jnp.float32,
        )

    acc[...] = jnp.zeros_like(acc)
    fill(0, 0, held[0])

    pl.semaphore_wait(barrier, count - 1)

    groups = arrival_groups(sizes)
    for number, (first, last) in enumerate(groups):
        for index in range(first, last):
            pltpu.make_async_remote_copy(
                src_ref=held.at[0],
                dst_ref=held.at[index],
                send_sem=send_sem,
                recv_sem=recv_sem.at[number],
                device_id=peers[index],
                device_id_type=MESH,
            ).start()

    def landed(first, last, sem):
        span = held.at[pl.ds(first, last - first)]
        return pltpu.make_async_copy(span, span, sem)

    def arrive(pair):
        for number, (first, last) in enumerate(groups):
            if first == 1:
                continue

            @pl.when(pair == first // 2)
            def _():
                landed(first, last, recv_sem.at[number]).wait()

    def advance(pair, buffer):
        arrive(pair)
        product(1 - buffer)
        fill(buffer, 0, held[2 * pair])
        fill(buffer, 1, held[2 * pair + 1])

    landed(1, 2, recv_sem.at[0]).wait()
    fill(0, 1, held[1])

    @pl.loop(0, count // 4 - 1)
    def _(quad):
        advance(2 * quad + 1, 1)
        advance(2 * quad + 2, 0)

    advance(count // 2 - 1, 1)
    product(1)

    top = blocks * pad
    folded = acc[: 2 * top, :] + acc[2 * top :, :]
    folded = folded[:, :LANES] + folded[:, LANES:]
    signs = jnp.concatenate([even, odd], axis=1).astype(jnp.bfloat16)
    spread_out = jnp.dot(halves([folded]), signs, preferred_element_type=jnp.float32)
    spread_out = spread_out[: 2 * top, :] + spread_out[2 * top :, :]
    evens, odds = spread_out[:, :LANES], spread_out[:, LANES:]
    z_re = evens[:top, :] - odds[top:, :]
    z_im = evens[top:, :] + odds[:top, :]
    for j in range(blocks):
        span = slice(j * LANES, (j + 1) * LANES)
        here = slice(j * pad, (j + 1) * pad)
        z = times((z_re[here, :], z_im[here, :]), gain_u)
        tile = z[0] * gain_v[0][:, span] - z[1] * gain_v[1][:, span]
        out_ref[:, span] = tile[:rows, :]

    landed(1, count, send_sem).wait()


def body(sizes, visibility, destination, tile_slot, offsets, taper):
    count = math.prod(sizes)
    vis_count = visibility.shape[0]
    rows = IMG // count
    pad = -(-rows // 16) * 16
    vmem = pl.BlockSpec(memory_space=pltpu.VMEM)
    return pl.pallas_call(
        functools.partial(kernel, sizes, rows),
        out_shape=jax.ShapeDtypeStruct((rows, IMG), jnp.float32),
        in_specs=[pl.BlockSpec(memory_space=pl.ANY)] * 5,
        out_specs=vmem,
        scratch_shapes=[
            pltpu.VMEM((2, vis_count), jnp.float32),
            pltpu.VMEM((1, vis_count), jnp.int32),
            pltpu.VMEM((1, vis_count), jnp.int32),
            pltpu.VMEM((2, vis_count), jnp.int32),
            pltpu.SMEM((SUP,), jnp.float32),
            pltpu.VMEM((count, 4, vis_count), jnp.float32),
            pltpu.VMEM((2, 4 * (IMG // LANES) * pad, 2 * vis_count), jnp.bfloat16),
            pltpu.VMEM((2, 2 * LANES, 2 * vis_count), jnp.bfloat16),
            pltpu.VMEM((4 * (IMG // LANES) * pad, 2 * LANES), jnp.float32),
            pltpu.SemaphoreType.DMA((5,)),
            pltpu.SemaphoreType.DMA,
            pltpu.SemaphoreType.DMA((len(arrival_groups(sizes)),)),
        ],
        compiler_params=pltpu.CompilerParams(collective_id=0, has_side_effects=True),
        name="direct_facet",
    )(
        visibility.T,
        destination.reshape(1, vis_count),
        tile_slot.reshape(1, vis_count),
        offsets.T,
        taper,
    )


def solution(mesh):
    return jax.shard_map(
        functools.partial(body, tuple(mesh.shape[name] for name in AXES)),
        mesh=mesh,
        in_specs=(P(AXES, None), P(AXES, None), P(AXES), P(AXES, None), P()),
        out_specs=P(AXES, None),
        check_vma=False,
    )
```
